32 devices in a mesh: dp: 8 (over y, x, core), mp: 4 (over z).
Axes of the slice: x: 2, y: 2, z: 4, core: 2. Of those that a mesh axis runs over, the one named last changes fastest.
Arguments:
- images: bfloat16 [1536, 1024], P('dp', 'mp'), may hold values from -80 to 80, as said below
- texts: bfloat16 [1536, 1024], P('dp', 'mp'), may hold values from -80 to 80, as said below
- logit_scale: float32 [1], replicated, may hold values from 240 to 300
Outputs:
- row_loss: float32 [1536], P('dp')
- column_loss: float32 [1536], P('dp')
The draws below stay inside these ranges and needn't reach their ends.
Inputs may be any that keep to these rules, and one draw needn't show every extreme that they name: `images`: Real-valued entries. `texts`: Real-valued entries.
All inputs are finite; a program needn't handle non-finite values.
Results may differ from the reference program's by a relative error of at most 0.0044.
Values may be sent and summed in bfloat16 or wider, within the bound.
A program may use at most 64 MiB of HBM per device.

```python
import jax
import jax.numpy as jnp
from jax import lax

D = 1024
ROWS_DEV = 192
BATCH = 1536
N_DP = 8


def draw_pair(key):
    image_key = jax.random.fold_in(key, 11)
    text_key = jax.random.fold_in(key, 12)
    common_key = jax.random.fold_in(key, 15)
    spread_key = jax.random.fold_in(key, 16)
    common = jax.random.normal(common_key, (1, D), jnp.float32)
    block_spread = jnp.exp(jax.random.uniform(spread_key, (BATCH // ROWS_DEV,), jnp.float32, jnp.log(0.03), 0.0))
    spread = block_spread[jnp.arange(BATCH) // ROWS_DEV][:, None]
    weight = jnp.sqrt(1.0 - spread * spread)
    image_rows = weight * common + spread * jax.random.normal(image_key, (BATCH, D), jnp.float32)
    text_rows = jax.random.normal(text_key, (BATCH, D), jnp.float32)
    image_rows = jnp.clip(image_rows, -80.0, 80.0)
    text_rows = jnp.clip(text_rows, -80.0, 80.0)
    return (image_rows, text_rows)


def draw_images(key, part):
    return draw_pair(key)[0].astype(jnp.bfloat16)


def draw_texts(key, part):
    return draw_pair(key)[1].astype(jnp.bfloat16)


def setup_inputs(seed: int = 0) -> dict:
    streams_of = jax.random.split(jax.random.key(seed), 4)
    return {
        "images": draw_images(jax.random.fold_in(streams_of[3], 71), 0),
        "texts": draw_texts(jax.random.fold_in(streams_of[3], 71), 0),
        "logit_scale": jnp.clip(jax.random.uniform(streams_of[2], (1,), jnp.float32, 240.0, 300.0), 240.0, 300.0),
    }


def normalize(rows):
    values = rows.astype(jnp.float32)
    return (values * lax.rsqrt(lax.optimization_barrier(jnp.sum(values * values, axis=1, keepdims=True)) + 1e-06)).astype(jnp.bfloat16)

def reference(images, texts, logit_scale):
    image_unit = normalize(images)
    text_unit = normalize(texts)
    inverse_temp = logit_scale[0]
    matched = inverse_temp * lax.optimization_barrier(jnp.sum(image_unit.astype(jnp.float32) * text_unit.astype(jnp.float32), axis=1))
    blocks = text_unit.reshape(N_DP, ROWS_DEV, D)

    def visit(states, block):
        row_top, row_total = states
        scores = inverse_temp * jnp.dot(block, image_unit.T, preferred_element_type=jnp.float32)
        column_top = lax.optimization_barrier(jnp.max(scores, axis=1))
        column_lse = column_top + jnp.log(lax.optimization_barrier(jnp.sum(jnp.exp(scores - column_top[:, None]), axis=1)))
        new_top = jnp.maximum(row_top, lax.optimization_barrier(jnp.max(scores, axis=0)))
        row_total = row_total * jnp.exp(row_top - new_top) + lax.optimization_barrier(jnp.sum(jnp.exp(scores - new_top[None, :]), axis=0))
        return ((new_top, row_total), column_lse)
    start = (jnp.full((BATCH,), -1e+30, jnp.float32), jnp.zeros((BATCH,), jnp.float32))
    (row_top, row_total), column_lse = lax.scan(visit, start, blocks)
    row_loss = row_top + jnp.log(row_total) - matched
    column_loss = column_lse.reshape(-1) - matched
    return (row_loss, column_loss)
```

```python
import functools

import jax
import jax.numpy as jnp
from jax import lax
from jax.experimental import pallas as pl
from jax.experimental.pallas import tpu as pltpu
from jax.sharding import PartitionSpec as P

F32 = jnp.float32
MESH = pl.DeviceIdType.MESH
CORES = 2
CHUNKS = 2


def dot_t(a, b):
    return lax.dot_general(a, b, (((1,), (1,)), ((), ())), preferred_element_type=F32)


def unit_slices(slices):
    wide = [s.astype(F32) for s in slices]
    square = functools.reduce(lambda p, q: p + q, [w * w for w in wide])
    inv = lax.rsqrt(jnp.sum(square, axis=1, keepdims=True) + 1e-06)
    return [(w * inv).astype(jnp.bfloat16) for w in wide]


def top_total(scores):
    top = jnp.max(scores, axis=0, keepdims=True)
    return top, jnp.sum(jnp.exp(scores - top), axis=0, keepdims=True)


def loss_kernel(
    groups,
    slices,
    scale_ref,
    img_hbm,
    txt_hbm,
    out_ref,
    img,
    txt,
    txt_out,
    row_msg,
    col_msg,
    row_got,
    col_got,
    load_sem,
    word,
    tz_send,
    tx_send,
    txt_recv,
    ir_send,
    il_send,
    ip_send,
    iz_recv,
    ip_recv,
    row_send,
    row_recv,
    col_send,
    col_recv,
):
    dp = lax.axis_index("dp")
    m = lax.axis_index("mp")
    h = dp // CORES
    c = dp % CORES
    partner = dp + 1 - 2 * c
    quarter = txt.shape[2]
    rows = out_ref.shape[1]
    spare = col_msg.shape[2] // 2

    load_txt = pltpu.make_async_copy(txt_hbm, txt_out, load_sem.at[0])
    load_own = pltpu.make_async_copy(txt_hbm.at[m], txt.at[m, h], load_sem.at[1])
    load_img = pltpu.make_async_copy(img_hbm, img.at[c, m], load_sem.at[2])
    load_txt.start()
    load_own.start()
    load_img.start()

    barrier = pltpu.get_barrier_semaphore()

    def group_peer(k):
        return lax.rem(h + k, groups)

    def slice_peer(k):
        return lax.rem(m + k, slices)

    def greet(to_dp, to_mp):
        pl.semaphore_signal(
            barrier, inc=1, device_id={"dp": to_dp, "mp": to_mp}, device_id_type=MESH
        )

    has_left = m >= 1
    has_right = m + 1 < slices
    left = jnp.maximum(m - 1, 0)
    right = jnp.minimum(m + 1, slices - 1)
    pl.when(has_left)(lambda: greet(dp, left))
    pl.when(has_right)(lambda: greet(dp, right))
    greet(partner, m)
    for k in range(1, groups):
        greet(group_peer(k) * CORES + c, m)
    pl.semaphore_wait(barrier, groups + has_left.astype(jnp.int32) + has_right.astype(jnp.int32))

    def send(src, dst, s_sem, r_sem, to_dp, to_mp):
        return pltpu.make_async_remote_copy(
            src_ref=src,
            dst_ref=dst,
            send_sem=s_sem,
            recv_sem=r_sem,
            device_id={"dp": to_dp, "mp": to_mp},
            device_id_type=MESH,
        )

    pending = []

    def go(copy):
        copy.start()
        pending.append((None, copy))

    load_img.wait()

    def pass_on(b, q, right, left):
        block = img.at[c, b, q]
        if right is not None:
            r = send(block, block, ir_send.at[b, q], iz_recv.at[b, q], dp, jnp.minimum(m + 1, slices - 1))
            pl.when(right)(r.start)
            pending.append((right, r))
        if left is not None:
            l = send(block, block, il_send.at[b, q], iz_recv.at[b, q], dp, jnp.maximum(m - 1, 0))
            pl.when(left)(l.start)
            pending.append((left, l))

    def to_partner(b, q):
        block = img.at[c, b, q]
        return send(block, block, ip_send.at[b, q], ip_recv.at[b, q], partner, m)

    for q in range(CHUNKS):
        pass_on(m, q, m + 1 < slices, m >= 1)
    load_txt.wait()
    def tell(to, sem):
        pl.semaphore_signal(
            sem, inc=1, device_id={"dp": dp, "mp": to}, device_id_type=MESH
        )

    def text_to(to, cond):
        copy = send(txt_out.at[to], txt.at[m, h], tz_send.at[to], txt_recv.at[m, h], dp, to)
        pl.when(cond)(copy.start)
        pending.append((cond, copy))

    for d in range(1, slices):
        if d > 1:
            pl.when(has_right & (m - (d - 1) >= 0))(lambda: tell(right, word.at[0]))
            pl.when(has_left & (m + (d - 1) < slices))(lambda: tell(left, word.at[1]))
            pl.when(m - d >= 0)(lambda: pl.semaphore_wait(word.at[0], 1))
            pl.when(m + d < slices)(lambda: pl.semaphore_wait(word.at[1], 1))
        text_to(jnp.maximum(m - d, 0), m - d >= 0)
        text_to(jnp.minimum(m + d, slices - 1), m + d < slices)

    def spread(s):
        for k in reversed(range(1, groups)):
            to = group_peer(k) * CORES + c
            go(send(txt.at[s, h], txt.at[s, h], tx_send.at[s, k], txt_recv.at[s, h], to, m))

    load_own.wait()
    spread(m)

    for q in range(CHUNKS):
        go(to_partner(m, q))

    def landed(ref, sem):
        pltpu.make_async_copy(ref, ref, sem).wait()

    def texts_in(k):
        s = slice_peer(k)
        landed(txt.at[s, h], txt_recv.at[s, h])
        spread(s)

    for k in range(1, slices):
        for q in range(CHUNKS):
            low = m - k
            high = m + k
            has_low = low >= 0
            has_high = high < slices
            low_i = jnp.maximum(low, 0)
            high_i = jnp.minimum(high, slices - 1)

            def take(b):
                landed(img.at[c, b, q], iz_recv.at[b, q])

            pl.when(has_low)(functools.partial(take, low_i))
            pass_on(low_i, q, jnp.logical_and(has_low, m + 1 < slices), None)
            pl.when(has_high)(functools.partial(take, high_i))
            pass_on(high_i, q, None, jnp.logical_and(has_high, m >= 1))
            low_p = to_partner(low_i, q)
            pl.when(has_low)(low_p.start)
            pending.append((has_low, low_p))
            high_p = to_partner(high_i, q)
            pl.when(has_high)(high_p.start)
            pending.append((has_high, high_p))

            if k == 1 and q == CHUNKS - 1:
                for j in range(1, slices):
                    texts_in(j)

    for k in range(1, groups):
        for s in range(slices):
            landed(txt.at[s, group_peer(k)], txt_recv.at[s, group_peer(k)])

    scale = scale_ref[0]
    width = txt.shape[3]
    text_unit = unit_slices([txt[s].reshape(groups * quarter, width) for s in range(slices)])

    def tile(which, own):
        unit = unit_slices([img[which, s].reshape(rows, width) for s in range(slices)])
        by_row = scale * functools.reduce(
            lambda p, q: p + q, [dot_t(t, u) for t, u in zip(text_unit, unit)]
        )
        by_col = scale * functools.reduce(
            lambda p, q: p + q, [dot_t(u, t) for t, u in zip(text_unit, unit)]
        )
        row_top, row_total = top_total(by_row)
        message = jnp.concatenate([row_top, row_total], axis=0)
        row_msg[which] = message
        for k in range(1 if own else 0, slices):
            to = slice_peer(k)
            go(
                send(
                    row_msg.at[which],
                    row_got.at[c, m],
                    row_send.at[which, k],
                    row_recv.at[c, m],
                    dp if own else partner,
                    to,
                )
            )
        if own:
            row_got[c, m] = message
            image_row = lax.broadcasted_iota(jnp.int32, by_col.shape, 0) - m * quarter
            text_row = lax.broadcasted_iota(jnp.int32, by_col.shape, 1) - h * quarter
            pair = (text_row == image_row) & (text_row >= 0) & (text_row < quarter)
            matched = jnp.sum(jnp.where(pair, by_col, 0.0), axis=0, keepdims=True)
            return top_total(by_col) + (matched,)
        return top_total(by_col)

    top_a, total_a, own_matched = tile(c, True)
    for s in range(slices):
        for q in range(CHUNKS):
            landed(img.at[1 - c, s, q], ip_recv.at[s, q])
    top_b, total_b = tile(1 - c, False)
    col_top = jnp.maximum(top_a, top_b)
    col_total = total_a * jnp.exp(top_a - col_top) + total_b * jnp.exp(top_b - col_top)
    for g in range(groups):
        part = slice(g * quarter, (g + 1) * quarter)
        col_msg[g, 0:2, 0:quarter] = jnp.concatenate([col_top[:, part], col_total[:, part]], axis=0)
        col_msg[g, 0:1, spare : spare + quarter] = own_matched[:, part]
    col_got[m, h] = col_msg[h]
    for k in reversed(range(groups)):
        g = group_peer(k)
        for j in range(slices):
            if k == 0 and j == 0:
                continue
            go(
                send(
                    col_msg.at[g],
                    col_got.at[m, h],
                    col_send.at[k, j],
                    col_recv.at[m, h],
                    g * CORES + c,
                    slice_peer(j),
                )
            )

    for k in range(slices):
        s = slice_peer(k)
        if k > 0:
            landed(row_got.at[c, s], row_recv.at[c, s])
        landed(row_got.at[1 - c, s], row_recv.at[1 - c, s])
    got = row_got[...].reshape(CORES * slices, *row_got.shape[2:])
    peak = jnp.max(got[:, 0, :], axis=0, keepdims=True)
    whole = jnp.sum(got[:, 1, :] * jnp.exp(got[:, 0, :] - peak), axis=0, keepdims=True)
    row_lse = peak + jnp.log(whole)

    for k in range(groups):
        g = group_peer(k)
        for j in range(slices):
            if k == 0 and j == 0:
                continue
            s = slice_peer(j)
            landed(col_got.at[s, g], col_recv.at[s, g])
    pieces = []
    pairs = []
    for s in range(slices):
        tops = col_got[s, :, 0, 0:quarter]
        totals = col_got[s, :, 1, 0:quarter]
        peak = jnp.max(tops, axis=0, keepdims=True)
        pieces.append(
            peak + jnp.log(jnp.sum(totals * jnp.exp(tops - peak), axis=0, keepdims=True))
        )
        pairs.append(jnp.sum(col_got[s, :, 0, spare : spare + quarter], axis=0, keepdims=True))
    matched = jnp.concatenate(pairs, axis=1)
    out_ref[...] = jnp.concatenate([row_lse, jnp.concatenate(pieces, axis=1)], axis=0) - matched

    for cond, copy in pending:
        if cond is None:
            copy.wait_send()
        else:
            pl.when(cond)(copy.wait_send)


def kernel_on_device(groups, slices, images, texts, logit_scale):
    rows, width = images.shape
    quarter = rows // slices
    lanes = 128 * pl.cdiv(2 * quarter, 128)
    dma = pltpu.SemaphoreType.DMA
    vmem = pl.BlockSpec(memory_space=pltpu.VMEM)
    hbm = pl.BlockSpec(memory_space=pl.ANY)
    losses = pl.pallas_call(
        functools.partial(loss_kernel, groups, slices),
        out_shape=pltpu.VMEM((2, rows), F32),
        in_specs=[pl.BlockSpec(memory_space=pltpu.SMEM), hbm, hbm],
        out_specs=vmem,
        scratch_shapes=[
            pltpu.VMEM((CORES, slices, CHUNKS, rows // CHUNKS, width), images.dtype),
            pltpu.VMEM((slices, groups, quarter, width), texts.dtype),
            pltpu.VMEM((slices, quarter, width), texts.dtype),
            pltpu.VMEM((CORES, 2, rows), F32),
            pltpu.VMEM((groups, 2, lanes), F32),
            pltpu.VMEM((CORES, slices, 2, rows), F32),
            pltpu.VMEM((slices, groups, 2, lanes), F32),
            dma((3,)),
            pltpu.SemaphoreType.REGULAR((2,)),
            dma((slices,)),
            dma((slices, groups)),
            dma((slices, groups)),
            dma((slices, CHUNKS)),
            dma((slices, CHUNKS)),
            dma((slices, CHUNKS)),
            dma((slices, CHUNKS)),
            dma((slices, CHUNKS)),
            dma((CORES, slices)),
            dma((CORES, slices)),
            dma((groups, slices)),
            dma((slices, groups)),
        ],
        compiler_params=pltpu.CompilerParams(collective_id=0, has_side_effects=True),
    )(
        logit_scale,
        images.reshape(CHUNKS, rows // CHUNKS, width),
        texts.reshape(slices, quarter, width),
    )
    return losses[0], losses[1]


def normalize(rows):
    values = rows.astype(F32)
    return (values * lax.rsqrt(jnp.sum(values * values, axis=1, keepdims=True) + 1e-06)).astype(
        jnp.bfloat16
    )


def collectives_on_device(images, texts, logit_scale):
    count = lax.axis_size("dp")
    m = lax.axis_index("mp")
    image_unit = normalize(lax.all_gather(images, "mp", axis=1, tiled=True))
    text_unit = normalize(lax.all_to_all(texts, "mp", split_axis=0, concat_axis=1, tiled=True))
    scale = logit_scale[0]
    quarter = text_unit.shape[0]
    mine = lax.dynamic_slice_in_dim(image_unit, m * quarter, quarter, 0)
    matched = scale * jnp.sum(mine.astype(F32) * text_unit.astype(F32), axis=1)
    scores = scale * dot_t(lax.all_gather(text_unit, "dp", axis=0, tiled=True), image_unit)
    row_top = jnp.max(scores, axis=0)
    row_total = jnp.sum(jnp.exp(scores - row_top[None, :]), axis=0)
    col_top = jnp.max(scores, axis=1)
    col_total = jnp.sum(jnp.exp(scores - col_top[:, None]), axis=1)
    got_top, got_total = (
        lax.all_to_all(v.reshape(count, quarter), "dp", split_axis=0, concat_axis=0, tiled=True)
        for v in (col_top, col_total)
    )
    col_peak = jnp.max(got_top, axis=0)
    col_lse = col_peak + jnp.log(jnp.sum(got_total * jnp.exp(got_top - col_peak[None, :]), axis=0))
    row_peak = lax.pmax(row_top, "mp")
    row_lse = row_peak + jnp.log(lax.psum(row_total * jnp.exp(row_top - row_peak), "mp"))
    col_full = lax.all_gather(col_lse, "mp", axis=0, tiled=True)
    matched_full = lax.all_gather(matched, "mp", axis=0, tiled=True)
    return row_lse - matched_full, col_full - matched_full


def solution(mesh):
    dp, mp = mesh.shape["dp"], mesh.shape["mp"]
    small = dp % CORES == 0 and dp * mp <= 64
    body = (
        functools.partial(kernel_on_device, dp // CORES, mp) if small else collectives_on_device
    )
    return jax.shard_map(
        body,
        mesh=mesh,
        in_specs=(P("dp", "mp"), P("dp", "mp"), P()),
        out_specs=(P("dp"), P("dp")),
        check_vma=False,
    )
```

```python
import functools

import jax
import jax.numpy as jnp
from jax import lax
from jax.experimental import pallas as pl
from jax.experimental.pallas import tpu as pltpu
from jax.sharding import PartitionSpec as P

F32 = jnp.float32
MESH = pl.DeviceIdType.MESH
CORES = 2
PLANE = 4
DEPTH = 4
CHUNKS = 2
OWN, NEAR, OTHER, FAR = range(4)
ACROSS_Z, ACROSS_X, ACROSS_Y, ACROSS_CORE, BEYOND = range(5)


def dot_t(a, b):
    return lax.dot_general(a, b, (((1,), (1,)), ((), ())), preferred_element_type=F32)


def top_total(scores):
    top = jnp.max(scores, axis=0, keepdims=True)
    return top, jnp.sum(jnp.exp(scores - top), axis=0, keepdims=True)


def squares(block):
    wide = block.astype(F32)
    square = wide * wide
    high = square.astype(jnp.bfloat16)
    low = (square - high.astype(F32)).astype(jnp.bfloat16)
    ones = jnp.ones((8, block.shape[1]), jnp.bfloat16)
    return dot_t(ones, high) + dot_t(ones, low), jnp.sum(square, axis=1, keepdims=True)


def loss_kernel(
    scale_ref,
    img_hbm,
    txt_hbm,
    out_ref,
    img,
    spare,
    txt,
    by_row,
    by_col,
    img_lane,
    txt_lane,
    img_sub,
    txt_sub,
    row_msg,
    col_msg,
    row_got,
    col_got,
    row_tally,
    col_tally,
    load_sem,
    img_recv,
    txt_recv,
    pair_recv,
    row_recv,
    col_recv,
    word,
    xy_send,
    pair_send,
    text_send,
    spare_send,
    row_send,
    col_send,
):
    dp = lax.axis_index("dp")
    m = lax.axis_index("mp")
    h = dp // CORES
    c = dp % CORES
    x = h % 2
    y = h // 2
    partner = dp + 1 - 2 * c
    beside = dp + CORES * (1 - 2 * x)
    above = dp + 2 * CORES * (1 - 2 * y)
    across = above + CORES * (1 - 2 * x)
    half = img.shape[2]
    rows = 2 * half

    low = DEPTH // 2 - 1
    inner = (m == low) | (m == low + 1)
    last = DEPTH - 1
    a = jnp.clip(m - low, 0, 1)
    other = last - m
    near = low + a
    far = last - near

    def signal(sem, to_dp, to_mp):
        pl.semaphore_signal(
            sem, inc=1, device_id={"dp": to_dp, "mp": to_mp}, device_id_type=MESH
        )

    def send(src, dst, s_sem, r_sem, to_dp, to_mp):
        pltpu.make_async_remote_copy(
            src_ref=src,
            dst_ref=dst,
            send_sem=s_sem,
            recv_sem=r_sem,
            device_id={"dp": to_dp, "mp": to_mp},
            device_id_type=MESH,
        ).start()

    def landed(ref, sem):
        pltpu.make_async_copy(ref, ref, sem).wait()

    load_text = pltpu.make_async_copy(txt_hbm, txt.at[OWN, 0], load_sem.at[0])
    load_spare = pltpu.make_async_copy(img_hbm, spare, load_sem.at[1])
    load_own = pltpu.make_async_copy(img_hbm.at[a], img.at[OWN, 0], load_sem.at[2])

    barrier = pltpu.get_barrier_semaphore()
    pl.when(m <= low)(lambda: signal(barrier, dp, jnp.minimum(m + 1, last)))
    pl.when(inner & (x == 0))(lambda: signal(barrier, beside, m))
    pl.when(inner & (y == 0))(lambda: signal(barrier, above, m))
    pl.when(inner & (c == 1))(lambda: signal(barrier, partner, m))
    load_spare.start()
    load_own.start()
    load_text.start()
    greeters = (m > 0).astype(jnp.int32) + jnp.where(inner, x + y + 1 - c, 0)
    pl.when(greeters > 0)(lambda: pl.semaphore_wait(barrier, greeters))
    pl.when(m == low + 1)(lambda: signal(barrier, dp, last))
    pl.when((m > 0) & inner)(lambda: signal(word.at[ACROSS_Z], dp, jnp.maximum(m - 1, 0)))
    pl.when(inner & (x == 1))(lambda: signal(word.at[ACROSS_X], beside, m))
    pl.when(inner & (y == 1))(lambda: signal(word.at[ACROSS_Y], above, m))
    pl.when(inner & (c == 0))(lambda: signal(word.at[ACROSS_CORE], partner, m))

    def hear(cond, which):
        pl.when(cond)(lambda: pl.semaphore_wait(word.at[which], 1))

    @pl.when(jnp.logical_not(inner))
    def _():
        hear(m == 0, ACROSS_Z)
        load_spare.wait()

        def halves_far():
            send(spare.at[1 - a], img.at[FAR, 0], spare_send, img_recv.at[FAR, 0], dp, far)

        def halves_near():
            send(spare.at[a], img.at[NEAR, 0], spare_send, img_recv.at[NEAR, 0], dp, near)

        pl.when(m != 0)(halves_far)
        halves_near()

        @pl.when(m == 0)
        def _():
            pl.semaphore_wait(word.at[BEYOND], 1)
            halves_far()

        load_text.wait()
        for q in range(CHUNKS):
            send(
                txt.at[OWN, 0, q], txt.at[NEAR, 0, q], text_send, txt_recv.at[NEAR, q], dp, near
            )
        load_own.wait()
        landed(spare, spare_send)
        landed(txt.at[OWN, 0], text_send)

    @pl.when(inner)
    def _():
        @pl.when(m == low)
        def _():
            pl.semaphore_wait(word.at[ACROSS_Z], 1)
            signal(word.at[BEYOND], dp, 0)

        load_spare.wait()
        send(spare.at[1 - a], img.at[OTHER, 0], spare_send, img_recv.at[OTHER, 0], dp, other)
        load_text.wait()
        for q in range(CHUNKS):
            send(
                txt.at[OWN, 0, q], txt.at[OTHER, 0, q], text_send, txt_recv.at[OTHER, q], dp, other
            )
        load_own.wait()

        def spread(p):
            send(img.at[p, 0], img.at[p, 1], xy_send, img_recv.at[p, 1], beside, m)
            send(img.at[p, 0], img.at[p, 2], xy_send, img_recv.at[p, 2], above, m)

        def relay(p):
            landed(img.at[p, 1 + c], img_recv.at[p, 1 + c])
            to = jnp.where(c == 0, above, beside)
            send(img.at[p, 1 + c], img.at[p, 3], xy_send, img_recv.at[p, 3], to, m)

        def texts_to_partner(p):
            send(txt.at[p, 0], txt.at[p, 1], pair_send, pair_recv.at[p], partner, m)

        def add(positions, first):
            lane_img, sub_img, lane_txt, sub_txt, rc, cr = ([] for _ in range(6))
            for p in positions:
                u = img[p].reshape(PLANE * half, img.shape[3])
                t = txt[p].reshape(CORES * rows, txt.shape[4])
                rc.append(dot_t(t, u))
                cr.append(dot_t(u, t))
                l, s = squares(u)
                lane_img.append(l)
                sub_img.append(s)
                l, s = squares(t)
                lane_txt.append(l)
                sub_txt.append(s)
            parts = []
            for ref, terms in (
                (by_row, rc),
                (by_col, cr),
                (img_lane, lane_img),
                (img_sub, sub_img),
                (txt_lane, lane_txt),
                (txt_sub, sub_txt),
            ):
                total = functools.reduce(lambda p, q: p + q, terms)
                parts.append(total if first else ref[...] + total)
            return parts

        hear(x == 0, ACROSS_X)
        hear(y == 0, ACROSS_Y)
        spread(OWN)
        hear(c == 1, ACROSS_CORE)
        texts_to_partner(OWN)

        relay(OWN)
        landed(img.at[OTHER, 0], img_recv.at[OTHER, 0])
        spread(OTHER)
        landed(img.at[NEAR, 0], img_recv.at[NEAR, 0])
        spread(NEAR)

        def forward(q):
            landed(txt.at[NEAR, 0, q], txt_recv.at[NEAR, q])
            send(txt.at[NEAR, 0, q], txt.at[FAR, 0, q], text_send, txt_recv.at[FAR, q], dp, other)

        forward(0)
        landed(img.at[OWN, 3], img_recv.at[OWN, 3])
        landed(img.at[FAR, 0], img_recv.at[FAR, 0])
        send(img.at[FAR, 0], img.at[FAR, 3], xy_send, img_recv.at[FAR, 3], across, m)
        spread(FAR)
        relay(OTHER)
        for q in range(1, CHUNKS):
            forward(q)
        texts_to_partner(NEAR)
        relay(NEAR)
        for q in range(CHUNKS):
            landed(txt.at[OTHER, 0, q], txt_recv.at[OTHER, q])
        texts_to_partner(OTHER)

        landed(img.at[OWN, 2 - c], img_recv.at[OWN, 2 - c])
        landed(txt.at[OWN, 1], pair_recv.at[OWN])
        for p in (OTHER, NEAR):
            landed(img.at[p, 2 - c], img_recv.at[p, 2 - c])
            landed(img.at[p, 3], img_recv.at[p, 3])
            landed(txt.at[p, 1], pair_recv.at[p])
        for ref, value in zip(
            (by_row, by_col, img_lane, img_sub, txt_lane, txt_sub),
            add((OWN, OTHER, NEAR), True),
        ):
            ref[...] = value

        for q in range(CHUNKS):
            landed(txt.at[FAR, 0, q], txt_recv.at[FAR, q])
        texts_to_partner(FAR)
        for k in range(1, PLANE):
            landed(img.at[FAR, k], img_recv.at[FAR, k])
        landed(txt.at[FAR, 1], pair_recv.at[FAR])

        rc, cr, lane_img, sub_img, lane_txt, sub_txt = add((FAR,), False)

        def inverse(total):
            return lax.rsqrt(total + 1e-06)

        scale = scale_ref[0]
        scores = rc * (scale * inverse(sub_txt)) * inverse(lane_img[0:1])
        row_top, row_total = top_total(scores)
        message = jnp.concatenate([row_top, row_total], axis=0)
        for k in range(PLANE):
            row_msg[k, :, 0:half] = message[:, k * half : (k + 1) * half]
        chips = (dp, beside, above, across)
        for z in range(DEPTH):
            for k in reversed(range(PLANE)):

                def row_to(k=k, z=z):
                    send(row_msg.at[k], row_got.at[a, k], row_send, row_recv, chips[k], z)

                if k:
                    row_to()
                else:
                    pl.when(m != z)(row_to)
        row_got[a, 0, :, 0:half] = message[:, 0:half]

        scores_own = scores[0:rows, 0:half]
        text_row = lax.broadcasted_iota(jnp.int32, scores_own.shape, 0) - a * half
        image_row = lax.broadcasted_iota(jnp.int32, scores_own.shape, 1)
        matched = jnp.sum(
            jnp.where(text_row == image_row, scores_own, 0.0), axis=0, keepdims=True
        )
        scores = cr * (scale * inverse(sub_img)) * inverse(lane_txt[0:1])
        message = jnp.concatenate(top_total(scores), axis=0)
        for k in range(CORES):
            col_msg[k, 0:2, 0:rows] = message[:, k * rows : (k + 1) * rows]
        col_msg[0, 2:3, 0:half] = matched
        for z in range(DEPTH):
            send(col_msg.at[1], col_got.at[a, 1], col_send, col_recv, partner, z)
            pl.when(m != z)(
                lambda: send(col_msg.at[0], col_got.at[a, 0], col_send, col_recv, dp, z)
            )
        col_got[a, 0, 0:2, 0:rows] = message[:, 0:rows]
        col_got[a, 0, 2:3, 0:half] = matched

        landed(img.at[0:3], xy_send)
        landed(img.at[0:2], pair_send)
        landed(img.at[0], text_send)
        landed(img.at[0, 0], spare_send)

    pl.when(inner)(lambda: landed(row_tally.at[0 : 2 * PLANE - 1], row_recv))
    pl.when(jnp.logical_not(inner))(lambda: landed(row_tally.at[0 : 2 * PLANE], row_recv))
    row_lse = []
    for w in range(2):
        tops = row_got[w, :, 0, 0:half]
        totals = row_got[w, :, 1, 0:half]
        peak = jnp.max(tops, axis=0, keepdims=True)
        row_lse.append(
            peak + jnp.log(jnp.sum(totals * jnp.exp(tops - peak), axis=0, keepdims=True))
        )
    pl.when(inner)(lambda: landed(col_tally.at[0:3], col_recv))
    pl.when(jnp.logical_not(inner))(lambda: landed(col_tally.at[0:4], col_recv))
    got = col_got[...].reshape(2 * CORES, *col_got.shape[2:])
    tops = got[:, 0, 0:rows]
    totals = got[:, 1, 0:rows]
    peak = jnp.max(tops, axis=0, keepdims=True)
    col_lse = peak + jnp.log(jnp.sum(totals * jnp.exp(tops - peak), axis=0, keepdims=True))
    matched = jnp.concatenate([col_got[w, 0, 2:3, 0:half] for w in range(2)], axis=1)
    out_ref[...] = jnp.concatenate([jnp.concatenate(row_lse, axis=1), col_lse], axis=0) - matched

    @pl.when(inner)
    def _():
        landed(row_tally.at[0 : DEPTH * PLANE - 1], row_send)
        landed(col_tally.at[0 : DEPTH * CORES - 1], col_send)


def kernel_on_device(images, texts, logit_scale):
    rows, width = images.shape
    half = rows // 2
    lanes = 128 * pl.cdiv(rows, 128)
    half_lanes = 128 * pl.cdiv(half, 128)
    wide_img = PLANE * half
    wide_txt = CORES * rows
    dma = pltpu.SemaphoreType.DMA
    vmem = pl.BlockSpec(memory_space=pltpu.VMEM)
    hbm = pl.BlockSpec(memory_space=pl.ANY)
    losses = pl.pallas_call(
        loss_kernel,
        out_shape=pltpu.VMEM((2, rows), F32),
        in_specs=[pl.BlockSpec(memory_space=pltpu.SMEM), hbm, hbm],
        out_specs=vmem,
        scratch_shapes=[
            pltpu.VMEM((DEPTH, PLANE, half, width), images.dtype),
            pltpu.VMEM((2, half, width), images.dtype),
            pltpu.VMEM((DEPTH, CORES, CHUNKS, rows // CHUNKS, width), texts.dtype),
            pltpu.VMEM((wide_txt, wide_img), F32),
            pltpu.VMEM((wide_img, wide_txt), F32),
            pltpu.VMEM((8, wide_img), F32),
            pltpu.VMEM((8, wide_txt), F32),
            pltpu.VMEM((wide_img, 1), F32),
            pltpu.VMEM((wide_txt, 1), F32),
            pltpu.VMEM((PLANE, 2, half_lanes), F32),
            pltpu.VMEM((CORES, 4, lanes), F32),
            pltpu.VMEM((2, PLANE, 2, half_lanes), F32),
            pltpu.VMEM((2, CORES, 4, lanes), F32),
            pltpu.VMEM((DEPTH * PLANE, 2, half_lanes), F32),
            pltpu.VMEM((DEPTH * CORES, 4, lanes), F32),
            dma((3,)),
            dma((DEPTH, PLANE)),
            dma((DEPTH, CHUNKS)),
            dma((DEPTH,)),
            dma(()),
            dma(()),
            pltpu.SemaphoreType.REGULAR((5,)),
            dma(()),
            dma(()),
            dma(()),
            dma(()),
            dma(()),
            dma(()),
        ],
        compiler_params=pltpu.CompilerParams(collective_id=0, has_side_effects=True),
    )(
        logit_scale,
        images.reshape(2, half, width),
        texts.reshape(CHUNKS, rows // CHUNKS, width),
    )
    return losses[0], losses[1]


def normalize(rows):
    values = rows.astype(F32)
    return (values * lax.rsqrt(jnp.sum(values * values, axis=1, keepdims=True) + 1e-06)).astype(
        jnp.bfloat16
    )


def collectives_on_device(images, texts, logit_scale):
    count = lax.axis_size("dp")
    m = lax.axis_index("mp")
    image_unit = normalize(lax.all_gather(images, "mp", axis=1, tiled=True))
    text_unit = normalize(lax.all_to_all(texts, "mp", split_axis=0, concat_axis=1, tiled=True))
    scale = logit_scale[0]
    quarter = text_unit.shape[0]
    mine = lax.dynamic_slice_in_dim(image_unit, m * quarter, quarter, 0)
    matched = scale * jnp.sum(mine.astype(F32) * text_unit.astype(F32), axis=1)
    scores = scale * dot_t(lax.all_gather(text_unit, "dp", axis=0, tiled=True), image_unit)
    row_top = jnp.max(scores, axis=0)
    row_total = jnp.sum(jnp.exp(scores - row_top[None, :]), axis=0)
    col_top = jnp.max(scores, axis=1)
    col_total = jnp.sum(jnp.exp(scores - col_top[:, None]), axis=1)
    got_top, got_total = (
        lax.all_to_all(v.reshape(count, quarter), "dp", split_axis=0, concat_axis=0, tiled=True)
        for v in (col_top, col_total)
    )
    col_peak = jnp.max(got_top, axis=0)
    col_lse = col_peak + jnp.log(jnp.sum(got_total * jnp.exp(got_top - col_peak[None, :]), axis=0))
    row_peak = lax.pmax(row_top, "mp")
    row_lse = row_peak + jnp.log(lax.psum(row_total * jnp.exp(row_top - row_peak), "mp"))
    col_full = lax.all_gather(col_lse, "mp", axis=0, tiled=True)
    matched_full = lax.all_gather(matched, "mp", axis=0, tiled=True)
    return row_lse - matched_full, col_full - matched_full


def solution(mesh):
    dp, mp = mesh.shape["dp"], mesh.shape["mp"]
    small = dp == CORES * PLANE and mp == DEPTH
    body = kernel_on_device if small else collectives_on_device
    return jax.shard_map(
        body,
        mesh=mesh,
        in_specs=(P("dp", "mp"), P("dp", "mp"), P()),
        out_specs=(P("dp"), P("dp")),
        check_vma=False,
    )
```

```python
import functools

import jax
import jax.numpy as jnp
from jax import lax
from jax.experimental import pallas as pl
from jax.experimental.pallas import tpu as pltpu
from jax.sharding import PartitionSpec as P

F32 = jnp.float32
MESH = pl.DeviceIdType.MESH
CORES = 2
PLANE = 4
DEPTH = 4
CHUNKS = 2
OWN, NEAR, OTHER, FAR = range(4)
ACROSS_Z, ACROSS_X, ACROSS_Y, ACROSS_CORE, BEYOND = range(5)


def dot_t(a, b):
    return lax.dot_general(a, b, (((1,), (1,)), ((), ())), preferred_element_type=F32)


def top_total(scores):
    top = jnp.max(scores, axis=0, keepdims=True)
    return top, jnp.sum(jnp.exp(scores - top), axis=0, keepdims=True)


def squares(block):
    wide = block.astype(F32)
    square = wide * wide
    high = square.astype(jnp.bfloat16)
    low = (square - high.astype(F32)).astype(jnp.bfloat16)
    ones = jnp.ones((8, block.shape[1]), jnp.bfloat16)
    return dot_t(ones, high) + dot_t(ones, low), jnp.sum(square, axis=1, keepdims=True)


def loss_kernel(
    scale_ref,
    img_hbm,
    txt_hbm,
    out_ref,
    img,
    spare,
    txt,
    by_row,
    by_col,
    img_lane,
    txt_lane,
    img_sub,
    txt_sub,
    row_msg,
    col_msg,
    row_got,
    col_got,
    row_tally,
    col_tally,
    load_sem,
    img_recv,
    txt_recv,
    pair_recv,
    row_recv,
    col_recv,
    word,
    xy_send,
    pair_send,
    text_send,
    spare_send,
    row_send,
    col_send,
):
    dp = lax.axis_index("dp")
    m = lax.axis_index("mp")
    h = dp // CORES
    c = dp % CORES
    x = h % 2
    y = h // 2
    partner = dp + 1 - 2 * c
    beside = dp + CORES * (1 - 2 * x)
    above = dp + 2 * CORES * (1 - 2 * y)
    across = above + CORES * (1 - 2 * x)
    half = img.shape[2]
    rows = 2 * half

    low = DEPTH // 2 - 1
    inner = (m == low) | (m == low + 1)
    last = DEPTH - 1
    a = jnp.clip(m - low, 0, 1)
    other = last - m
    near = low + a
    far = last - near

    def signal(sem, to_dp, to_mp):
        pl.semaphore_signal(
            sem, inc=1, device_id={"dp": to_dp, "mp": to_mp}, device_id_type=MESH
        )

    def send(src, dst, s_sem, r_sem, to_dp, to_mp):
        pltpu.make_async_remote_copy(
            src_ref=src,
            dst_ref=dst,
            send_sem=s_sem,
            recv_sem=r_sem,
            device_id={"dp": to_dp, "mp": to_mp},
            device_id_type=MESH,
        ).start()

    def landed(ref, sem):
        pltpu.make_async_copy(ref, ref, sem).wait()

    load_text = pltpu.make_async_copy(txt_hbm, txt.at[OWN, 0], load_sem.at[0])
    load_spare = pltpu.make_async_copy(img_hbm, spare, load_sem.at[1])
    load_own = pltpu.make_async_copy(img_hbm.at[a], img.at[OWN, 0], load_sem.at[2])

    barrier = pltpu.get_barrier_semaphore()
    pl.when(m <= low)(lambda: signal(barrier, dp, jnp.minimum(m + 1, last)))
    pl.when(inner & (x == 0))(lambda: signal(barrier, beside, m))
    pl.when(inner & (y == 0))(lambda: signal(barrier, above, m))
    pl.when(inner & (c == 1))(lambda: signal(barrier, partner, m))
    load_spare.start()
    load_own.start()
    load_text.start()
    greeters = (m > 0).astype(jnp.int32) + jnp.where(inner, x + y + 1 - c, 0)
    pl.when(greeters > 0)(lambda: pl.semaphore_wait(barrier, greeters))
    pl.when(m == low + 1)(lambda: signal(barrier, dp, last))
    pl.when((m > 0) & inner)(lambda: signal(word.at[ACROSS_Z], dp, jnp.maximum(m - 1, 0)))
    pl.when(inner & (x == 1))(lambda: signal(word.at[ACROSS_X], beside, m))
    pl.when(inner & (y == 1))(lambda: signal(word.at[ACROSS_Y], above, m))
    pl.when(inner & (c == 0))(lambda: signal(word.at[ACROSS_CORE], partner, m))

    def hear(cond, which):
        pl.when(cond)(lambda: pl.semaphore_wait(word.at[which], 1))

    @pl.when(jnp.logical_not(inner))
    def _():
        hear(m == 0, ACROSS_Z)
        load_spare.wait()

        def halves_far():
            send(spare.at[1 - a], img.at[FAR, 0], spare_send, img_recv.at[FAR, 0], dp, far)

        def halves_near():
            send(spare.at[a], img.at[NEAR, 0], spare_send, img_recv.at[NEAR, 0], dp, near)

        pl.when(m != 0)(halves_far)
        halves_near()

        @pl.when(m == 0)
        def _():
            pl.semaphore_wait(word.at[BEYOND], 1)
            halves_far()

        load_text.wait()
        for q in range(CHUNKS):
            send(
                txt.at[OWN, 0, q], txt.at[NEAR, 0, q], text_send, txt_recv.at[NEAR, q], dp, near
            )
        load_own.wait()
        landed(spare, spare_send)
        landed(txt.at[OWN, 0], text_send)

    @pl.when(inner)
    def _():
        def texts_to_partner(p):
            send(txt.at[p, 0], txt.at[p, 1], pair_send, pair_recv.at[p], partner, m)

        def cross(p):
            send(img.at[p, 0], img.at[p, 3], xy_send, img_recv.at[p, 3], across, m)

        def spread(p):
            send(img.at[p, 0], img.at[p, 1], xy_send, img_recv.at[p, 1], beside, m)
            send(img.at[p, 0], img.at[p, 2], xy_send, img_recv.at[p, 2], above, m)

        load_own.wait()
        hear(x == 0, ACROSS_X)
        hear(y == 0, ACROSS_Y)
        signal(word.at[BEYOND], beside, m)
        spread(OWN)

        @pl.when(m == low)
        def _():
            pl.semaphore_wait(word.at[ACROSS_Z], 1)
            signal(word.at[BEYOND], dp, 0)

        load_spare.wait()
        send(spare.at[1 - a], img.at[OTHER, 0], spare_send, img_recv.at[OTHER, 0], dp, other)
        load_text.wait()
        for q in range(CHUNKS):
            send(
                txt.at[OWN, 0, q], txt.at[OTHER, 0, q], text_send, txt_recv.at[OTHER, q], dp, other
            )
        pl.semaphore_wait(word.at[BEYOND], 1)
        cross(OWN)
        hear(c == 1, ACROSS_CORE)
        texts_to_partner(OWN)

        def pass_on(p):
            landed(img.at[p, 0], img_recv.at[p, 0])
            cross(p)
            spread(p)

        def forward(q):
            landed(txt.at[NEAR, 0, q], txt_recv.at[NEAR, q])
            send(txt.at[NEAR, 0, q], txt.at[FAR, 0, q], text_send, txt_recv.at[FAR, q], dp, other)

        def complete(p):
            for k in range(1, PLANE):
                landed(img.at[p, k], img_recv.at[p, k])
            landed(txt.at[p, 1], pair_recv.at[p])

        def terms(p):
            u = img[p].reshape(PLANE * half, img.shape[3])
            t = txt[p].reshape(CORES * rows, txt.shape[4])
            return (dot_t(t, u), dot_t(u, t)) + squares(u) + squares(t)

        totals = (by_row, by_col, img_lane, img_sub, txt_lane, txt_sub)

        pass_on(OTHER)
        pass_on(NEAR)
        forward(0)
        pass_on(FAR)
        for q in range(1, CHUNKS):
            forward(q)
        texts_to_partner(NEAR)
        for q in range(CHUNKS):
            landed(txt.at[OTHER, 0, q], txt_recv.at[OTHER, q])
        texts_to_partner(OTHER)

        complete(OWN)
        for ref, term in zip(totals, terms(OWN)):
            ref[...] = term
        for p in (OTHER, NEAR):
            complete(p)
            for ref, term in zip(totals, terms(p)):
                ref[...] += term

        for q in range(CHUNKS):
            landed(txt.at[FAR, 0, q], txt_recv.at[FAR, q])
        texts_to_partner(FAR)
        complete(FAR)
        rc, cr, lane_img, sub_img, lane_txt, sub_txt = (
            ref[...] + term for ref, term in zip(totals, terms(FAR))
        )

        def inverse(total):
            return lax.rsqrt(total + 1e-06)

        scale = scale_ref[0]
        scores = rc * (scale * inverse(sub_txt)) * inverse(lane_img[0:1])
        row_top, row_total = top_total(scores)
        message = jnp.concatenate([row_top, row_total], axis=0)
        for k in range(PLANE):
            row_msg[k, :, 0:half] = message[:, k * half : (k + 1) * half]
        chips = (dp, beside, above, across)
        for z in range(DEPTH):
            for k in reversed(range(PLANE)):

                def row_to(k=k, z=z):
                    send(row_msg.at[k], row_got.at[a, k], row_send, row_recv, chips[k], z)

                if k:
                    row_to()
                else:
                    pl.when(m != z)(row_to)
        row_got[a, 0, :, 0:half] = message[:, 0:half]

        scores_own = scores[0:rows, 0:half]
        text_row = lax.broadcasted_iota(jnp.int32, scores_own.shape, 0) - a * half
        image_row = lax.broadcasted_iota(jnp.int32, scores_own.shape, 1)
        matched = jnp.sum(
            jnp.where(text_row == image_row, scores_own, 0.0), axis=0, keepdims=True
        )
        scores = cr * (scale * inverse(sub_img)) * inverse(lane_txt[0:1])
        message = jnp.concatenate(top_total(scores), axis=0)
        for k in range(CORES):
            col_msg[k, 0:2, 0:rows] = message[:, k * rows : (k + 1) * rows]
        col_msg[0, 2:3, 0:half] = matched
        for z in range(DEPTH):
            send(col_msg.at[1], col_got.at[a, 1], col_send, col_recv, partner, z)
            pl.when(m != z)(
                lambda: send(col_msg.at[0], col_got.at[a, 0], col_send, col_recv, dp, z)
            )
        col_got[a, 0, 0:2, 0:rows] = message[:, 0:rows]
        col_got[a, 0, 2:3, 0:half] = matched

        landed(img.at[0:3], xy_send)
        landed(img.at[0:2], pair_send)
        landed(img.at[0], text_send)
        landed(img.at[0, 0], spare_send)

    pl.when(inner)(lambda: landed(row_tally.at[0 : 2 * PLANE - 1], row_recv))
    pl.when(jnp.logical_not(inner))(lambda: landed(row_tally.at[0 : 2 * PLANE], row_recv))
    row_lse = []
    for w in range(2):
        tops = row_got[w, :, 0, 0:half]
        totals = row_got[w, :, 1, 0:half]
        peak = jnp.max(tops, axis=0, keepdims=True)
        row_lse.append(
            peak + jnp.log(jnp.sum(totals * jnp.exp(tops - peak), axis=0, keepdims=True))
        )
    pl.when(inner)(lambda: landed(col_tally.at[0:3], col_recv))
    pl.when(jnp.logical_not(inner))(lambda: landed(col_tally.at[0:4], col_recv))
    got = col_got[...].reshape(2 * CORES, *col_got.shape[2:])
    tops = got[:, 0, 0:rows]
    totals = got[:, 1, 0:rows]
    peak = jnp.max(tops, axis=0, keepdims=True)
    col_lse = peak + jnp.log(jnp.sum(totals * jnp.exp(tops - peak), axis=0, keepdims=True))
    matched = jnp.concatenate([col_got[w, 0, 2:3, 0:half] for w in range(2)], axis=1)
    out_ref[...] = jnp.concatenate([jnp.concatenate(row_lse, axis=1), col_lse], axis=0) - matched

    @pl.when(inner)
    def _():
        landed(row_tally.at[0 : DEPTH * PLANE - 1], row_send)
        landed(col_tally.at[0 : DEPTH * CORES - 1], col_send)


def kernel_on_device(images, texts, logit_scale):
    rows, width = images.shape
    half = rows // 2
    lanes = 128 * pl.cdiv(rows, 128)
    half_lanes = 128 * pl.cdiv(half, 128)
    wide_img = PLANE * half
    wide_txt = CORES * rows
    dma = pltpu.SemaphoreType.DMA
    vmem = pl.BlockSpec(memory_space=pltpu.VMEM)
    hbm = pl.BlockSpec(memory_space=pl.ANY)
    losses = pl.pallas_call(
        loss_kernel,
        out_shape=pltpu.VMEM((2, rows), F32),
        in_specs=[pl.BlockSpec(memory_space=pltpu.SMEM), hbm, hbm],
        out_specs=vmem,
        scratch_shapes=[
            pltpu.VMEM((DEPTH, PLANE, half, width), images.dtype),
            pltpu.VMEM((2, half, width), images.dtype),
            pltpu.VMEM((DEPTH, CORES, CHUNKS, rows // CHUNKS, width), texts.dtype),
            pltpu.VMEM((wide_txt, wide_img), F32),
            pltpu.VMEM((wide_img, wide_txt), F32),
            pltpu.VMEM((8, wide_img), F32),
            pltpu.VMEM((8, wide_txt), F32),
            pltpu.VMEM((wide_img, 1), F32),
            pltpu.VMEM((wide_txt, 1), F32),
            pltpu.VMEM((PLANE, 2, half_lanes), F32),
            pltpu.VMEM((CORES, 4, lanes), F32),
            pltpu.VMEM((2, PLANE, 2, half_lanes), F32),
            pltpu.VMEM((2, CORES, 4, lanes), F32),
            pltpu.VMEM((DEPTH * PLANE, 2, half_lanes), F32),
            pltpu.VMEM((DEPTH * CORES, 4, lanes), F32),
            dma((3,)),
            dma((DEPTH, PLANE)),
            dma((DEPTH, CHUNKS)),
            dma((DEPTH,)),
            dma(()),
            dma(()),
            pltpu.SemaphoreType.REGULAR((5,)),
            dma(()),
            dma(()),
            dma(()),
            dma(()),
            dma(()),
            dma(()),
        ],
        compiler_params=pltpu.CompilerParams(collective_id=0, has_side_effects=True),
    )(
        logit_scale,
        images.reshape(2, half, width),
        texts.reshape(CHUNKS, rows // CHUNKS, width),
    )
    return losses[0], losses[1]


def normalize(rows):
    values = rows.astype(F32)
    return (values * lax.rsqrt(jnp.sum(values * values, axis=1, keepdims=True) + 1e-06)).astype(
        jnp.bfloat16
    )


def collectives_on_device(images, texts, logit_scale):
    count = lax.axis_size("dp")
    m = lax.axis_index("mp")
    image_unit = normalize(lax.all_gather(images, "mp", axis=1, tiled=True))
    text_unit = normalize(lax.all_to_all(texts, "mp", split_axis=0, concat_axis=1, tiled=True))
    scale = logit_scale[0]
    quarter = text_unit.shape[0]
    mine = lax.dynamic_slice_in_dim(image_unit, m * quarter, quarter, 0)
    matched = scale * jnp.sum(mine.astype(F32) * text_unit.astype(F32), axis=1)
    scores = scale * dot_t(lax.all_gather(text_unit, "dp", axis=0, tiled=True), image_unit)
    row_top = jnp.max(scores, axis=0)
    row_total = jnp.sum(jnp.exp(scores - row_top[None, :]), axis=0)
    col_top = jnp.max(scores, axis=1)
    col_total = jnp.sum(jnp.exp(scores - col_top[:, None]), axis=1)
    got_top, got_total = (
        lax.all_to_all(v.reshape(count, quarter), "dp", split_axis=0, concat_axis=0, tiled=True)
        for v in (col_top, col_total)
    )
    col_peak = jnp.max(got_top, axis=0)
    col_lse = col_peak + jnp.log(jnp.sum(got_total * jnp.exp(got_top - col_peak[None, :]), axis=0))
    row_peak = lax.pmax(row_top, "mp")
    row_lse = row_peak + jnp.log(lax.psum(row_total * jnp.exp(row_top - row_peak), "mp"))
    col_full = lax.all_gather(col_lse, "mp", axis=0, tiled=True)
    matched_full = lax.all_gather(matched, "mp", axis=0, tiled=True)
    return row_lse - matched_full, col_full - matched_full


def solution(mesh):
    dp, mp = mesh.shape["dp"], mesh.shape["mp"]
    small = dp == CORES * PLANE and mp == DEPTH
    body = kernel_on_device if small else collectives_on_device
    return jax.shard_map(
        body,
        mesh=mesh,
        in_specs=(P("dp", "mp"), P("dp", "mp"), P()),
        out_specs=(P("dp"), P("dp")),
        check_vma=False,
    )
```
